32 devices in a mesh: row: 8 (over z, x), col: 4 (over y, core).
Axes of the slice: x: 2, y: 2, z: 4, core: 2. Of those that a mesh axis runs over, the one named last changes fastest.
Arguments:
- gradients: bfloat16 [32, 2, 524288], P(('row', 'col')), may hold values from -96 to 96
- master_params: float32 [2, 524288], P(None, ('row', 'col')), may hold values from -0.1 to 0.1
- first_moment: float32 [2, 524288], P(None, ('row', 'col')), may hold values from -3 to 3
- second_moment: float32 [2, 524288], P(None, ('row', 'col')), may hold values from 0.05 to 5
Outputs:
- new_master: float32 [2, 524288], P(None, ('row', 'col'))
- new_first: float32 [2, 524288], P(None, ('row', 'col'))
- new_second: float32 [2, 524288], P(None, ('row', 'col'))
- new_weights: bfloat16 [2, 524288], replicated
The draws below stay inside these ranges and needn't reach their ends.
All inputs are finite; a program needn't handle non-finite values.
Results may differ from the reference program's by a relative error of at most 0.009.
Values may be sent and summed in bfloat16 or wider, within the bound.
A program may use at most 64 MiB of HBM per device.

```python
import math
import jax
import jax.numpy as jnp
from jax import lax

LAYERS = 2
SLICE = 524288
DEVICES = 32


def spiked(result, rng, source, target, shards_of, factor):
    owner, partner = [(jnp.arange(result.shape[axis_at]) // (result.shape[axis_at] // shards_of)).reshape([-1 if axis == axis_at else 1 for axis in range(result.ndim)]) for axis_at in (source, target)]
    chosen = jax.random.permutation(rng, shards_of)[partner]
    strong = (owner == chosen) | (owner == (partner + shards_of // 2) % shards_of)
    return jnp.where(strong, factor * result, result)


def level_of(own_key, extent, split, smallest, largest):
    factor_of, own = 1.0, jax.random.fold_in(own_key, 6)
    for position, parts in split:
        heights = jnp.exp(jax.random.uniform(jax.random.fold_in(own, position), (parts,), jnp.float32, smallest / len(split), largest / len(split)))
        factor_of = factor_of * jnp.repeat(heights, extent[position] // parts).reshape([-1 if axis == position else 1 for axis in range(len(extent))])
    return factor_of


def gaussian(rng, dims, spread, most, split=(), held_as=jnp.bfloat16):
    result = jax.random.normal(rng, dims, jnp.float32) * spread
    if len(split) > 0:
        result = level_of(rng, dims, split, -0.22, 0.18) * result
    return jnp.clip(result, min=-most, max=most).astype(held_as)


def heavy_noise(own_key, dims, spread, bound, pieces, heavy, kind=jnp.bfloat16):
    drawn = spread * jax.random.normal(own_key, dims, jnp.float32)
    if pieces:
        drawn = drawn * level_of(own_key, dims, pieces, -0.22, 0.18)
    return jnp.clip(spiked(drawn, jax.random.fold_in(own_key, 3), *heavy), -bound, bound).astype(kind)


def setup_inputs(seed: int = 0) -> dict:
    splits = jax.random.split(jax.random.key(seed), 5)
    gradients = heavy_noise(splits[0], (DEVICES, LAYERS, SLICE), 16.0, 96.0, ((0, 32),), (0, 2, 32, 2.75))
    master_params = gaussian(splits[1], (LAYERS, SLICE), 0.025, 0.1, ((1, 32),), jnp.float32)
    first_moment = gaussian(splits[2], (LAYERS, SLICE), 0.5, 3.0, ((1, 32),), jnp.float32)
    second_moment = jnp.clip(jnp.exp(math.log(5.0) - 4.6051702 * jax.random.uniform(splits[3], (LAYERS, SLICE), jnp.float32) ** level_of(splits[3], (LAYERS, SLICE), ((1, 32),), -0.2, 0.2)), 0.05, 5.0)
    return {"gradients": gradients, "master_params": master_params, "first_moment": first_moment, "second_moment": second_moment}


beta_one = 0.9
beta_two = 0.95
learn_rate = 0.001
decay_rate = 0.1
epsilon = 1e-08
adam_step = 10.0

def adam_update(mean_grad, master_params, first_moment, second_moment):
    new_first = beta_one * first_moment + (1.0 - beta_one) * mean_grad
    new_second = beta_two * second_moment + (1.0 - beta_two) * mean_grad * mean_grad
    first_hat = new_first / (1.0 - beta_one ** adam_step)
    second_hat = new_second / (1.0 - beta_two ** adam_step)
    new_master = master_params - learn_rate * (first_hat / (jnp.sqrt(second_hat) + epsilon) + decay_rate * master_params)
    return (new_master, new_first, new_second)

def reference(gradients, master_params, first_moment, second_moment):
    mean_grad = lax.optimization_barrier(jnp.sum(gradients, axis=0, dtype=jnp.float32)) / DEVICES
    new_master, new_first, new_second = adam_update(mean_grad, master_params, first_moment, second_moment)
    return (new_master, new_first, new_second, new_master.astype(jnp.bfloat16))
```

```python
import functools
import heapq

import jax
import jax.numpy as jnp
import numpy as np
from jax import lax
from jax.experimental import pallas as pl
from jax.experimental.pallas import tpu as pltpu
from jax.sharding import PartitionSpec as P

beta_one = 0.9
beta_two = 0.95
learn_rate = 0.001
decay_rate = 0.1
epsilon = 1e-08
adam_step = 10.0

LANES = 128
FLOWS = ((32, "xyz", "zyx"), (32, "yxz", "yxz"), (24, "zyx", "zxy"), (32, "zyx", "zxy"), (24, "xyz", "zyx"), (40, "xyz", "zxy"), (32, "yzx", "yzx"), (8, "xyz", "zyx"), (8, "xyz", "xyz"), (24, "xyz", "zxy"))
FIRST = (7.2, 103.1, 65.1, -21.2, 31.4, 17.8, 17.5, 33.2, 70.7, 62.1)
STAGE = {('r', 1, 'far'): -116.4, ('r', 1, 'near'): 33.5, ('r', 2, 'far'): -41.5, ('r', 2, 'near'): 1.4, ('r', 2, 'all'): -109.3, ('r', 1, 'all'): -2.1, ('r', 3, 'all'): -41.2, ('g', -1, 0): -37.9, ('g', -1, 1): 89.8, ('g', 0, 1): 0.7, ('g', -1, 2): 82.8, ('g', 0, 2): -7.7, ('g', 1, 2): 16.8, ('g', -1, 3): -21.5, ('g', 0, 3): 76.6, ('g', 1, 3): -54.4, ('g', 2, 3): -60.5}
STEP_ROWS = 8
VMEM_LIMIT = 40 * 1024 * 1024
MESH = pl.DeviceIdType.MESH
CORE_RATE, CORE_LATENCY = 680e3, 1.0
LINK_RATE, LINK_LATENCY, HOP_LATENCY = 46.6e3, 2.2, 0.8
AHEAD = 0.3
STEP = 0.05


def adam_update(mean_grad, master_params, first_moment, second_moment):
    new_first = beta_one * first_moment + (1.0 - beta_one) * mean_grad
    new_second = beta_two * second_moment + (1.0 - beta_two) * mean_grad * mean_grad
    first_hat = new_first / (1.0 - beta_one**adam_step)
    second_hat = new_second / (1.0 - beta_two**adam_step)
    new_master = master_params - learn_rate * (
        first_hat / (jnp.sqrt(second_hat) + epsilon) + decay_rate * master_params
    )
    return (new_master, new_first, new_second)


def factors(n):
    out = []
    while n > 1:
        k = next(k for k in (4, 2, *range(3, n + 1)) if n % k == 0)
        out.append(k)
        n //= k
    return out


def digits_of(rows, cols):
    core = [2] if cols % 2 == 0 else []
    found = []
    for axis, sizes in (("row", factors(rows)), ("col", factors(cols // (2 if core else 1)) + core)):
        stride = int(np.prod(sizes, dtype=np.int64))
        for size in sizes:
            stride //= size
            found.append((axis, size, stride))
    return found


def order_of(digits, name):
    last = len(digits) - 1
    row_at = [i for i in range(last) if digits[i][0] == "row"]
    col_at = [i for i in range(last) if digits[i][0] == "col"]
    groups = {"x": row_at[-1:], "y": col_at[:1], "z": col_at[1:] + row_at[:-1]}
    return [i for letter in name for i in groups[letter]]


class Plan:
    def __init__(self, sizes, flows, first, stage_rank):
        self.sizes, self.flows, self.count = sizes, flows, len(sizes)
        self.first, self.stage_rank = first, stage_rank
        self.messages = {}
        self.build()
        self.simulate()

    def parts(self, f, p):
        order = self.flows[f][0]
        if 0 < p < self.count - 1 and self.sizes[order[p + 1]] == 2:
            return ("far", "near")
        return ("all",)

    def gather_unit(self, f, source, s):
        return ("g", f, s, source if s == 1 else None)

    def rank(self, key):
        f = key[1]
        if key[0] == "r":
            return self.first[f % len(self.first)] + self.stage_rank.get(("r", key[2], key[3]), 0.0)
        return self.first[f % len(self.first)] + self.stage_rank.get(("g", key[2], key[3]), 0.0)

    def cost(self, digit, size_bytes):
        size = self.sizes[digit]
        if digit == self.count - 1:
            return size_bytes * (size - 1) / CORE_RATE, CORE_LATENCY
        lanes = (size // 2) * (size - size // 2)
        return size_bytes * lanes / LINK_RATE, LINK_LATENCY + HOP_LATENCY * (size - 2)

    def build(self):
        sizes, count = self.sizes, self.count
        blocks = lambda digits: int(np.prod([sizes[i] for i in digits], dtype=np.int64))
        for f, (down, up, rows) in enumerate(self.flows):
            for p in range(count):
                parts = self.parts(f, p)
                for part in parts:
                    needs = set()
                    for q in range(p):
                        back = self.parts(f, q)
                        needs.add(("r", f, q, back[0] if q == p - 1 else back[-1]))
                    self.messages["r", f, p, part] = (
                        down[p], blocks(down[p + 1 :]) // len(parts) * rows, needs, ("r", f, p, part)
                    )
            for s in range(count):
                for k in range(-1, s):
                    held = 1 if k < 0 else (sizes[up[k]] - 1) * blocks(up[:k])
                    needs = {("u", f)} if k < 0 else {self.gather_unit(f, j, k) for j in range(-1, k)}
                    if k >= 0:
                        needs = set(needs)
                    self.messages["g", f, k, s] = (up[s], held * rows, needs, self.gather_unit(f, k, s))

    def simulate(self):
        waiting = {key: set(message[2]) for key, message in self.messages.items()}
        users = {}
        for key, needs in waiting.items():
            for unit in needs:
                users.setdefault(unit, []).append(key)
        coming = {}
        for key, message in self.messages.items():
            coming[message[3]] = coming.get(message[3], 0) + 1
        sums = {f: {u for u in coming if u[0] == "r" and u[1] == f} for f in range(len(self.flows))}
        free, events, pending, lands = {}, [], [], {}
        self.actions = []
        serial = 0
        clock = 0.0

        def ready(key):
            heapq.heappush(pending, (self.rank(key), key[1], self.serials[key], key))

        self.serials = {key: i for i, key in enumerate(self.messages)}
        for key, needs in waiting.items():
            if not needs:
                ready(key)

        def dispatch():
            nonlocal serial
            again = []
            while pending:
                item = heapq.heappop(pending)
                key = item[3]
                digit, amount, _, unit = self.messages[key]
                if free.get(digit, 0.0) > clock + AHEAD:
                    again.append(item)
                    continue
                took, latency = self.cost(digit, amount * LANES * 2)
                free[digit] = max(clock, free.get(digit, 0.0)) + took
                self.actions.append(("send",) + key)
                lands[unit] = max(lands.get(unit, 0.0), free[digit] + latency)
                coming[unit] -= 1
                serial += 1
                if coming[unit] == 0:
                    heapq.heappush(events, (lands[unit], serial, unit))
                else:
                    heapq.heappush(events, (free[digit], serial, None))
                serial += 1
                heapq.heappush(events, (max(clock, free[digit] - AHEAD), serial, None))
            for item in again:
                heapq.heappush(pending, item)

        def arrive(unit):
            nonlocal clock
            f = unit[1]
            for key in users.get(unit, ()):
                waiting[key].discard(unit)
                if not waiting[key]:
                    ready(key)
            if unit[0] == "r":
                sums[f].discard(unit)
                if not sums[f]:
                    self.actions.append(("update", f))
                    clock += 0.1
                    arrive(("u", f))
                    self.actions.append(("store", f))

        dispatch()
        while events:
            at, _, unit = heapq.heappop(events)
            clock = max(clock, at)
            if unit is not None:
                self.actions.append(("wait",) + unit)
                clock += STEP
                arrive(unit)
            dispatch()
        assert not pending
        self.finish = clock


def kernel(digits, plan, rows, flat, grad, master, first, second, new_master, new_first, new_second, weights, scratch):
    sizes, count = plan.sizes, plan.count
    devices = int(np.prod(sizes))
    core = count - 1
    at = {axis: lax.axis_index(axis) for axis in ("row", "col")}
    mine = [lax.rem(at[axis] // stride, size) for axis, size, stride in digits]

    def peer(digit, t):
        axis, size, stride = digits[digit]
        value = lax.rem(mine[digit] + t, size)
        ids = dict(at)
        ids[axis] = at[axis] + (value - mine[digit]) * stride
        return value, (ids["row"], ids["col"])

    raw = scratch["raw"]
    for t in range(sizes[core] - 1, -1, -1):
        for i in range(sizes[0]):
            where = (i,) + (slice(None),) * (count - 2) + (peer(core, t)[0],)
            pltpu.make_async_copy(grad.at[where], raw.at[t, i], scratch["load_sem"].at[t]).start()
    for i, src in enumerate((master, first, second)):
        pltpu.make_async_copy(src, scratch["state"].at[i], scratch["load_sem"].at[sizes[core]]).start()

    barrier = pltpu.get_barrier_semaphore()
    greeted = 0
    for digit in range(count):
        for t in range(1, sizes[digit]):
            pl.semaphore_signal(barrier, inc=1, device_id=peer(digit, t)[1], device_id_type=MESH)
            greeted += 1
    pl.semaphore_wait(barrier, greeted)

    def loaded(t):
        ref = scratch["state"] if t == sizes[core] else raw.at[t]
        pltpu.make_async_copy(ref, ref, scratch["load_sem"].at[t]).wait()

    for t in range(sizes[core] - 1, -1, -1):
        loaded(t)

    units = {}

    def recv_sem(unit):
        return scratch["recv_sem"].at[units.setdefault(unit, len(units))]

    def send(phase, unit, src, dst, device):
        pltpu.make_async_remote_copy(
            src_ref=src,
            dst_ref=dst,
            send_sem=scratch["send_sem"].at[phase],
            recv_sem=recv_sem(unit),
            device_id=device,
            device_id_type=MESH,
        ).start()

    def wait(unit, ref):
        pltpu.make_async_remote_copy(
            src_ref=ref,
            dst_ref=ref,
            send_sem=scratch["send_sem"].at[0],
            recv_sem=recv_sem(unit),
            device_id=peer(core, 1)[1],
            device_id_type=MESH,
        ).wait_recv()

    def got_index(f, p, place):
        order = plan.flows[f][0]
        return tuple(place.get(i, mine[i]) for i in sorted(order[p + 1 :]))

    def total(f, p, place):
        order = plan.flows[f][0]
        value = raw[(0,) + tuple(place.get(i, mine[i]) for i in range(core)) + (rows[f],)].astype(jnp.float32)
        for q in range(p):
            for t in range(sizes[order[q]] - 1):
                value += scratch[f"got{f}_{q}"][(t,) + got_index(f, q, place)].astype(jnp.float32)
        return value

    def part_index(f, p, part):
        order = plan.flows[f][0]
        after = sorted(order[p + 1 :])
        if part == "all":
            return tuple(slice(None) for _ in after)
        fixed = peer(order[p + 1], 1 if part == "far" else 0)[0]
        return tuple(fixed if i == order[p + 1] else slice(None) for i in after)

    def scatter(f, p, part):
        order = plan.flows[f][0]
        digit = order[p]
        after = sorted(order[p + 1 :])
        for t in range(1, sizes[digit]):
            value, device = peer(digit, t)
            index = (t - 1,) + part_index(f, p, part)
            if p == 0:
                src = raw.at[(t,) + (slice(None),) * core + (rows[f],)]
            else:
                free = [i for i in after if part == "all" or i != order[p + 1]]
                for idx in np.ndindex(*(sizes[i] for i in free)):
                    place = dict(zip(free, idx))
                    place[digit] = value
                    if part != "all":
                        place[order[p + 1]] = peer(order[p + 1], 1 if part == "far" else 0)[0]
                    slot = (t - 1,) + tuple(place[i] for i in after)
                    scratch[f"sum{f}_{p}"][slot] = total(f, p, place).astype(jnp.bfloat16)
                src = scratch[f"sum{f}_{p}"].at[index]
            send(0, ("r", f, p, part), src, scratch[f"got{f}_{p}"].at[index], device)

    def forward(f, stage, s):
        order = plan.flows[f][1]
        digit = order[s]
        places = [{}]
        if stage >= 0:
            places = [{order[stage]: peer(order[stage], t)[0]} for t in range(1, sizes[order[stage]])]
        for place in places:
            where = tuple(
                slice(None) if i in order[: max(stage, 0)] else place.get(i, mine[i]) for i in range(count)
            ) + (rows[f],)
            for t in range(1, sizes[digit]):
                send(1, plan.gather_unit(f, stage, s), weights.at[where], weights.at[where], peer(digit, t)[1])

    def arrived(unit):
        f = unit[1]
        if unit[0] == "r":
            _, f, p, part = unit
            wait(unit, scratch[f"got{f}_{p}"].at[(slice(None),) + part_index(f, p, part)])
        else:
            _, f, s, source = unit
            order = plan.flows[f][1]
            where = [0] * count
            where[order[s]] = pl.ds(0, sizes[order[s]] - 1)
            for i in order[:s] if source is None else order[: max(source, 0)]:
                where[i] = slice(None)
            if source is not None and source >= 0:
                where[order[source]] = pl.ds(0, sizes[order[source]] - 1)
            wait(unit, weights.at[tuple(where) + (rows[f],)])

    states_ready = False
    results = {}
    for action in plan.actions:
        kind, rest = action[0], action[1:]
        if kind == "wait":
            arrived(rest)
        elif kind == "send":
            (scatter if rest[0] == "r" else forward)(*rest[1:])
        elif kind == "update":
            (f,) = rest
            if not states_ready:
                loaded(sizes[core])
                states_ready = True
            results[f] = adam_update(
                total(f, count, {}) / devices, *(scratch["state"][i, rows[f], :] for i in range(3))
            )
            weights[tuple(mine) + (rows[f],)] = results[f][0].astype(jnp.bfloat16)
        else:
            (f,) = rest
            for ref, value in zip((new_master, new_first, new_second), results.pop(f)):
                ref[rows[f], :] = value
    for phase in range(2):
        ref = flat.at[pl.ds(0, devices - 1)]
        pltpu.make_async_copy(ref, ref, scratch["send_sem"].at[phase]).wait()


def to_rows(x):
    layers, length = x.shape
    return x.reshape(layers, length // LANES, LANES).transpose(1, 0, 2).reshape(layers * length // LANES, LANES)


def from_rows(x, layers):
    total = x.shape[0]
    return x.reshape(total // layers, layers, LANES).transpose(1, 0, 2).reshape(layers, total // layers * LANES)


def write_out(*arrays):
    count = len(arrays)

    def body(*refs):
        copies = [pltpu.make_async_copy(refs[i], refs[count + i], refs[-1].at[i]) for i in range(count)]
        for copy in copies[::-1]:
            copy.start()
        for copy in copies:
            copy.wait()

    return pl.pallas_call(
        body,
        name="write_out",
        out_shape=tuple(jax.ShapeDtypeStruct(x.shape, x.dtype) for x in arrays),
        in_specs=[pl.BlockSpec(memory_space=pltpu.VMEM)] * count,
        out_specs=(pl.BlockSpec(memory_space=pltpu.HBM),) * count,
        scratch_shapes=[pltpu.SemaphoreType.DMA((count,))],
        compiler_params=pltpu.CompilerParams(vmem_limit_bytes=1 << 20),
    )(*arrays)


def shards(digits, gradients, master_params, first_moment, second_moment):
    count = len(digits)
    sizes = tuple(d[1] for d in digits)
    devices = int(np.prod(sizes))
    layers = gradients.shape[1]
    grad = to_rows(gradients[0])
    block = grad.shape[0] // devices
    core = count - 1
    whole, start, done = sum(share for share, _, _ in FLOWS), 0, 0
    flows, rows = [], []
    for share, down, up in FLOWS:
        done += share
        end = block if done == whole else done * block // whole // STEP_ROWS * STEP_ROWS
        if end > start:
            flows.append(([core] + order_of(digits, down), order_of(digits, up) + [core], end - start))
            rows.append(pl.ds(start, end - start))
            start = end
    plan = Plan(sizes, flows, FIRST, STAGE)

    scratch = {
        "load_sem": pltpu.SemaphoreType.DMA((sizes[-1] + 1,)),
        "send_sem": pltpu.SemaphoreType.DMA((2,)),
        "recv_sem": pltpu.SemaphoreType.DMA((sum(a[0] == "wait" for a in plan.actions),)),
        "state": pltpu.VMEM((3, block, LANES), jnp.float32),
        "raw": pltpu.VMEM((sizes[-1],) + sizes[:-1] + (block, LANES), jnp.bfloat16),
    }
    for f, (order, _, count_rows) in enumerate(flows):
        for p in range(count):
            after = tuple(sizes[i] for i in sorted(order[p + 1 :])) + (count_rows, LANES)
            if p > 0:
                scratch[f"sum{f}_{p}"] = pltpu.VMEM((sizes[order[p]] - 1,) + after, jnp.bfloat16)
            scratch[f"got{f}_{p}"] = pltpu.VMEM((sizes[order[p]] - 1,) + after, jnp.bfloat16)

    hbm_spec = pl.BlockSpec(memory_space=pltpu.HBM)
    vmem_spec = pl.BlockSpec(memory_space=pltpu.VMEM)
    part = jax.ShapeDtypeStruct((block, LANES), jnp.float32)
    names = list(scratch)

    def body(*refs):
        kernel(digits, plan, rows, *refs[:9], dict(zip(names, refs[9:])))

    new_master, new_first, new_second, weights = pl.pallas_call(
        body,
        name="average_update",
        out_shape=(part, part, part, jax.ShapeDtypeStruct(sizes + (block, LANES), jnp.bfloat16)),
        in_specs=[hbm_spec] * 5,
        out_specs=(vmem_spec,) * 4,
        scratch_shapes=[scratch[name] for name in names],
        compiler_params=pltpu.CompilerParams(
            collective_id=0, has_side_effects=True, vmem_limit_bytes=VMEM_LIMIT
        ),
    )(
        *(
            pltpu.with_memory_space_constraint(x, pltpu.HBM)
            for x in (
                grad.reshape((devices, block, LANES)),
                grad.reshape(sizes + (block, LANES)),
                to_rows(master_params),
                to_rows(first_moment),
                to_rows(second_moment),
            )
        )
    )
    results = write_out(new_master, new_first, new_second, weights.reshape(devices * block, LANES))
    return tuple(from_rows(x, layers) for x in results)


def solution(mesh):
    digits = digits_of(mesh.shape["row"], mesh.shape["col"])
    in_specs = (
        P(("row", "col"), None, None),
        P(None, ("row", "col")),
        P(None, ("row", "col")),
        P(None, ("row", "col")),
    )
    out_specs = (P(None, ("row", "col")), P(None, ("row", "col")), P(None, ("row", "col")), P())
    return jax.shard_map(
        functools.partial(shards, digits), mesh=mesh, in_specs=in_specs, out_specs=out_specs, check_vma=False
    )
```

```python
import functools
import heapq
import itertools

import jax
import jax.numpy as jnp
import numpy as np
from jax import lax
from jax.experimental import pallas as pl
from jax.experimental.pallas import tpu as pltpu
from jax.sharding import PartitionSpec as P

beta_one = 0.9
beta_two = 0.95
learn_rate = 0.001
decay_rate = 0.1
epsilon = 1e-08
adam_step = 10.0

LANES = 128
STEP_ROWS = 8
VMEM_LIMIT = 40 * 1024 * 1024
MESH = pl.DeviceIdType.MESH

FLOWS = (
    (16, "awb", "wz", (693.4, 364.7), (1, 1, 1), 0),
    (16, "yxz", "zw", (630.4, 654.7), (1, 0, 1), 1),
    (16, "wab", "yzx", (923.8, 248.4), (1, 0, 0), 0),
    (32, "yxz", "zw", (861.6, 445.6), (1, 0, 0), 1),
    (24, "xzy", "wba", (1104.1, 56.1), (0, 1, 1), 0),
    (24, "yxz", "zw", (643.2, 405.4), (1, 1, 0), 1),
    (16, "abw", "bwa", (245.7, 411.5), (0, 1, 0), 0),
    (32, "zw", "bwa", (612.6, 45.4), (0, 0, 0), 0),
    (24, "xyz", "zw", (273.2, 227.3), (0, 0, 0), 1),
    (16, "wz", "zw", (-58.2, 40.6), (1, 1, 1), 0),
    (24, "yxz", "zxy", (646.9, 317.3), (1, 0, 0), 0),
    (16, "awb", "wz", (903.8, 397.2), (1, 1, 1), 1),
)
DOWN_RANK = (
    (-257.8, -75.4, -87.6),
    (-198.2, 130.7, -438.3),
    (228.3, 352.9, 365.2),
    (34.2, -353.5, 32.8),
    (260.2, 128.6, -278.8),
    (183.4, 404.6, 16.4),
)
UP_RANK = (
    (4.9, 222.6, 48.8, -180.0, -50.9, -289.6),
    (-98.2, -171.0, 93.8, 44.2, 62.5, -43.2),
    (1.1, 130.9, -63.1, 261.5, 62.2, 292.1),
    (-45.6, -180.1, -151.6, 23.7, -62.6, 216.6),
    (-55.6, -121.9, -85.9, 148.8, 104.4, 184.5),
    (52.0, 107.0, -33.2, -57.9, 133.2, 105.4),
    (-49.2, -73.1, 181.0, -9.3, -56.4, -141.6),
)
RATE = 46.6e3
COST = {
    "x": ({"x": 1}, 2.2),
    "y": ({"y": 1}, 2.2),
    "a": ({"e": 1}, 2.2),
    "b": ({"e": 1, "m": 2}, 3.0),
    "z": ({"e": 3, "m": 4}, 3.8),
    "w": ({"x": 2, "y": 2}, 3.0),
    "c": ({"c": 46.6 / 680}, 1.0),
}
AHEAD, STEP, UPDATE = 0.3, 0.05, 0.1


def adam_update(mean_grad, master_params, first_moment, second_moment):
    new_first = beta_one * first_moment + (1.0 - beta_one) * mean_grad
    new_second = beta_two * second_moment + (1.0 - beta_two) * mean_grad * mean_grad
    first_hat = new_first / (1.0 - beta_one**adam_step)
    second_hat = new_second / (1.0 - beta_two**adam_step)
    new_master = master_params - learn_rate * (
        first_hat / (jnp.sqrt(second_hat) + epsilon) + decay_rate * master_params
    )
    return (new_master, new_first, new_second)


def factors(n):
    out, k = [], 2
    while n > 1:
        while n % k:
            k += 1
        out.append(k)
        n //= k
    return out


def digits_of(rows, cols):
    core = [2] if cols % 2 == 0 else [1]
    found = []
    for axis, sizes in (("row", factors(rows)), ("col", factors(cols // core[0]) + core)):
        stride = int(np.prod(sizes, dtype=np.int64))
        for size in sizes:
            stride //= size
            found.append((axis, size, stride))
    return found


def stages_of(digits):
    core = len(digits) - 1
    row_at = [i for i in range(core) if digits[i][0] == "row"]
    col_at = [i for i in range(core) if digits[i][0] == "col"]
    x, y, b, a = row_at[2:], col_at[:2], row_at[:1], row_at[1:2] + col_at[2:]
    return {"x": x, "y": y, "a": a, "b": b, "z": b + a, "w": x + y, "c": [core]}


class Plan:
    def __init__(self, sizes, groups, flows):
        self.sizes, self.groups, self.flows = sizes, groups, flows
        self.messages = {}
        self.build()
        self.simulate()

    def size(self, letters):
        return int(np.prod([self.sizes[i] for letter in letters for i in self.groups[letter]], dtype=np.int64))

    def parts(self, f, p):
        down = self.flows[f].down
        if 0 < p < len(down) - 1 and self.size(down[p + 1]) == 2 and self.flows[f].split[p]:
            return ("far", "near")
        return ("all",)

    def gather_unit(self, f, k, s):
        return ("g", f, s, k if self.flows[f].fine and 0 < s < len(self.flows[f].up) - 2 else None)

    def build(self):
        for f, flow in enumerate(self.flows):
            down, up = flow.down, flow.up
            for p in range(len(down)):
                parts = self.parts(f, p)
                needs = [("r", f, q, self.parts(f, q)[0 if q == p - 1 else -1]) for q in range(p)]
                for i, part in enumerate(parts):
                    rank = flow.first[0] + DOWN_RANK[p][i if len(parts) > 1 else 2]
                    amount = self.size(down[p + 1 :]) // len(parts) * flow.rows
                    self.messages["r", f, p, part] = (down[p], amount, rank, set(needs), ("r", f, p, part))
            for s in range(len(up)):
                for k in range(-1, s):
                    held = 1 if k < 0 else (self.size(up[k]) - 1) * self.size(up[:k])
                    needs = [("u", f)] if k < 0 else [self.gather_unit(f, j, k) for j in range(-1, k)]
                    rank = flow.first[1] + UP_RANK[k + 1][s]
                    self.messages["g", f, k, s] = (up[s], held * flow.rows, rank, set(needs), self.gather_unit(f, k, s))

    def simulate(self):
        serial = {key: i for i, key in enumerate(self.messages)}
        needs = {key: set(message[3]) for key, message in self.messages.items()}
        users, coming = {}, {}
        self.blocks = {}
        for key, (letter, amount, _, need, unit) in self.messages.items():
            for other in need:
                users.setdefault(other, []).append(key)
            coming[unit] = coming.get(unit, 0) + 1
            self.blocks[unit] = self.blocks.get(unit, 0) + amount // self.flows[key[1]].rows * (self.size(letter) - 1)
        sums = {f: {u for u in coming if u[:2] == ("r", f)} for f in range(len(self.flows))}
        free, lands, events, pending, order = {}, {}, [], [], itertools.count()
        self.actions = []
        clock = 0.0

        def ready(key):
            heapq.heappush(pending, (self.messages[key][2], key[1], serial[key], key))

        def dispatch():
            later = []
            while pending:
                item = heapq.heappop(pending)
                letter, amount, _, _, unit = self.messages[item[3]]
                links, latency = COST[letter]
                if any(free.get(link, 0.0) > clock + AHEAD for link in links):
                    later.append(item)
                    continue
                end = 0.0
                for link, units in links.items():
                    free[link] = max(clock, free.get(link, 0.0)) + amount * units * LANES * 2 / RATE
                    end = max(end, free[link])
                self.actions.append(("send",) + item[3])
                lands[unit] = max(lands.get(unit, 0.0), end + latency)
                coming[unit] -= 1
                if coming[unit] == 0:
                    heapq.heappush(events, (lands[unit], next(order), unit))
                for link in links:
                    heapq.heappush(events, (max(clock, free[link] - AHEAD), next(order), None))
            for item in later:
                heapq.heappush(pending, item)

        def arrive(unit):
            for key in users.get(unit, ()):
                needs[key].discard(unit)
                if not needs[key]:
                    ready(key)

        for key, need in needs.items():
            if not need:
                ready(key)
        dispatch()
        while events:
            at, _, unit = heapq.heappop(events)
            clock = max(clock, at)
            updated = None
            if unit is not None:
                self.actions.append(("wait",) + unit)
                clock += STEP
                arrive(unit)
                f = unit[1]
                if unit[0] == "r":
                    sums[f].discard(unit)
                    if not sums[f]:
                        self.actions.append(("update", f))
                        clock += UPDATE
                        arrive(("u", f))
                        updated = f
            dispatch()
            if updated is not None:
                self.actions.append(("store", updated))
        self.finish = clock


class Flow:
    def __init__(self, down, up, start, rows, first, split, fine):
        self.down, self.up, self.start, self.rows = down, up, start, rows
        self.first, self.split, self.fine = first, split, fine


def kernel(digits, plan, flat, grad, master, first, second, new_master, new_first, new_second, weights, scratch):
    sizes, groups, count = plan.sizes, plan.groups, len(plan.sizes)
    devices = int(np.prod(sizes))
    core = count - 1
    at = {axis: lax.axis_index(axis) for axis in ("row", "col")}
    mine = [lax.rem(at[axis] // stride, size) for axis, size, stride in digits]
    rows = [pl.ds(flow.start, flow.rows) for flow in plan.flows]

    def value(digit, t):
        return lax.rem(mine[digit] + t, sizes[digit]) if t else mine[digit]

    def offsets(letter):
        return list(itertools.product(*(range(sizes[i]) for i in groups[letter])))[1:]

    def place_of(letter, offset):
        return {i: value(i, t) for i, t in zip(groups[letter], offset)}

    def device_of(place):
        ids = dict(at)
        for i, new in place.items():
            axis, _, stride = digits[i]
            ids[axis] = ids[axis] + (new - mine[i]) * stride
        return (ids["row"], ids["col"])

    raw = scratch["raw"]
    for t in range(sizes[core] - 1, -1, -1):
        for i in range(sizes[0]):
            where = (i,) + (slice(None),) * (count - 2) + (value(core, t),)
            pltpu.make_async_copy(grad.at[where], raw.at[t, i], scratch["load_sem"].at[t]).start()
    for i, src in enumerate((master, first, second)):
        pltpu.make_async_copy(src, scratch["state"].at[i], scratch["load_sem"].at[sizes[core]]).start()

    barrier = pltpu.get_barrier_semaphore()
    greeted = {}
    for letter in sorted({letter for flow in plan.flows for letter in flow.down + flow.up}):
        for offset in offsets(letter):
            known = tuple((i, t) for i, t in zip(groups[letter], offset) if t)
            greeted[tuple(sorted(known))] = device_of(place_of(letter, offset))
    for device in greeted.values():
        pl.semaphore_signal(barrier, inc=1, device_id=device, device_id_type=MESH)
    pl.semaphore_wait(barrier, len(greeted))

    def loaded(t):
        ref = scratch["state"] if t == sizes[core] else raw.at[t]
        pltpu.make_async_copy(ref, ref, scratch["load_sem"].at[t]).wait()

    for t in range(sizes[core] - 1, -1, -1):
        loaded(t)

    units = {}

    def recv_sem(unit):
        return scratch["recv_sem"].at[units.setdefault(unit, len(units))]

    def send(phase, unit, src, dst, device):
        pltpu.make_async_remote_copy(
            src_ref=src,
            dst_ref=dst,
            send_sem=scratch["send_sem"].at[phase],
            recv_sem=recv_sem(unit),
            device_id=device,
            device_id_type=MESH,
        ).start()

    def arrived(unit):
        ref = flat.at[pl.ds(0, plan.blocks[unit]), rows[unit[1]]]
        pltpu.make_async_copy(ref, ref, recv_sem(unit)).wait()

    def after(f, p):
        return sorted(i for letter in plan.flows[f].down[p + 1 :] for i in groups[letter])

    def total(f, p, place):
        down = plan.flows[f].down
        found = raw[(0,) + tuple(place.get(i, mine[i]) for i in range(core)) + (rows[f],)].astype(jnp.float32)
        for q in range(p):
            index = tuple(place.get(i, mine[i]) for i in after(f, q))
            for t in range(plan.size(down[q]) - 1):
                found += scratch[f"got{f}_{q}"][(t,) + index].astype(jnp.float32)
        return found

    def scatter(f, p, part):
        down = plan.flows[f].down
        fixed = {}
        if part != "all":
            (digit,) = groups[down[p + 1]]
            fixed = {digit: value(digit, 1 if part == "far" else 0)}
        for slot, offset in enumerate(offsets(down[p])):
            place = place_of(down[p], offset)
            index = (slot,) + tuple(fixed.get(i, slice(None)) for i in after(f, p))
            if p == 0:
                src = raw.at[offset + (slice(None),) * core + (rows[f],)]
            else:
                free = [i for i in after(f, p) if i not in fixed]
                for idx in np.ndindex(*(sizes[i] for i in free)):
                    here = {**place, **fixed, **dict(zip(free, idx))}
                    at_slot = (slot,) + tuple(here[i] for i in after(f, p))
                    scratch[f"sum{f}_{p}"][at_slot] = total(f, p, here).astype(jnp.bfloat16)
                src = scratch[f"sum{f}_{p}"].at[index]
            send(0, ("r", f, p, part), src, scratch[f"got{f}_{p}"].at[index], device_of(place))

    def forward(f, k, s):
        up = plan.flows[f].up
        free = {i: slice(None) for letter in up[: max(k, 0)] for i in groups[letter]}
        places = [{}]
        if k >= 0:
            group = groups[up[k]]
            places = [
                {**free, group[j]: value(group[j], t), **{i: slice(None) for i in group[j + 1 :]}}
                for j in range(len(group))
                for t in range(1, sizes[group[j]])
            ]
        for place in places:
            ref = weights.at[tuple(place.get(i, mine[i]) for i in range(count)) + (rows[f],)]
            for offset in offsets(up[s]):
                send(1, plan.gather_unit(f, k, s), ref, ref, device_of(place_of(up[s], offset)))

    states_ready = False
    results = {}
    for action in plan.actions:
        kind, rest = action[0], action[1:]
        if kind == "wait":
            arrived(rest)
        elif kind == "send":
            (scatter if rest[0] == "r" else forward)(*rest[1:])
        elif kind == "update":
            (f,) = rest
            if not states_ready:
                loaded(sizes[core])
                states_ready = True
            results[f] = adam_update(
                total(f, len(plan.flows[f].down), {}) / devices, *(scratch["state"][i, rows[f], :] for i in range(3))
            )
            weights[tuple(mine) + (rows[f],)] = results[f][0].astype(jnp.bfloat16)
        else:
            (f,) = rest
            for ref, result in zip((new_master, new_first, new_second), results.pop(f)):
                ref[rows[f], :] = result
    for phase in range(2):
        ref = flat.at[pl.ds(0, devices - 1)]
        pltpu.make_async_copy(ref, ref, scratch["send_sem"].at[phase]).wait()


def to_rows(x):
    layers, length = x.shape
    return x.reshape(layers, length // LANES, LANES).transpose(1, 0, 2).reshape(layers * length // LANES, LANES)


def from_rows(x, layers):
    total = x.shape[0]
    return x.reshape(total // layers, layers, LANES).transpose(1, 0, 2).reshape(layers, total // layers * LANES)


def write_out(*arrays):
    count = len(arrays)

    def body(*refs):
        copies = [pltpu.make_async_copy(refs[i], refs[count + i], refs[-1].at[i]) for i in range(count)]
        for copy in copies[::-1]:
            copy.start()
        for copy in copies:
            copy.wait()

    return pl.pallas_call(
        body,
        name="write_out",
        out_shape=tuple(jax.ShapeDtypeStruct(x.shape, x.dtype) for x in arrays),
        in_specs=[pl.BlockSpec(memory_space=pltpu.VMEM)] * count,
        out_specs=(pl.BlockSpec(memory_space=pltpu.HBM),) * count,
        scratch_shapes=[pltpu.SemaphoreType.DMA((count,))],
        compiler_params=pltpu.CompilerParams(vmem_limit_bytes=1 << 20),
    )(*arrays)


def shards(digits, gradients, master_params, first_moment, second_moment):
    sizes = tuple(d[1] for d in digits)
    groups = stages_of(digits)
    devices = int(np.prod(sizes))
    layers = gradients.shape[1]
    grad = to_rows(gradients[0])
    block = grad.shape[0] // devices
    whole, start, done = sum(flow[0] for flow in FLOWS), 0, 0
    flows = []
    for share, down, up, first, split, fine in FLOWS:
        done += share
        end = block if done == whole else done * block // whole // STEP_ROWS * STEP_ROWS
        if end > start:
            down = [letter for letter in "c" + down if groups[letter]]
            up = [letter for letter in up + "c" if groups[letter]]
            flows.append(Flow(down, up, start, end - start, first, (0,) + split, fine))
            start = end
    plan = Plan(sizes, groups, flows)

    scratch = {
        "load_sem": pltpu.SemaphoreType.DMA((sizes[-1] + 1,)),
        "send_sem": pltpu.SemaphoreType.DMA((2,)),
        "recv_sem": pltpu.SemaphoreType.DMA((sum(action[0] == "wait" for action in plan.actions),)),
        "state": pltpu.VMEM((3, block, LANES), jnp.float32),
        "raw": pltpu.VMEM((sizes[-1],) + sizes[:-1] + (block, LANES), jnp.bfloat16),
    }
    for f, flow in enumerate(flows):
        for p, letter in enumerate(flow.down):
            after = sorted(i for other in flow.down[p + 1 :] for i in groups[other])
            shape = (plan.size(letter) - 1,) + tuple(sizes[i] for i in after) + (flow.rows, LANES)
            if p > 0:
                scratch[f"sum{f}_{p}"] = pltpu.VMEM(shape, jnp.bfloat16)
            scratch[f"got{f}_{p}"] = pltpu.VMEM(shape, jnp.bfloat16)

    hbm_spec = pl.BlockSpec(memory_space=pltpu.HBM)
    vmem_spec = pl.BlockSpec(memory_space=pltpu.VMEM)
    part = jax.ShapeDtypeStruct((block, LANES), jnp.float32)
    names = list(scratch)

    def body(*refs):
        kernel(digits, plan, *refs[:9], dict(zip(names, refs[9:])))

    new_master, new_first, new_second, weights = pl.pallas_call(
        body,
        name="average_update",
        out_shape=(part, part, part, jax.ShapeDtypeStruct(sizes + (block, LANES), jnp.bfloat16)),
        in_specs=[hbm_spec] * 5,
        out_specs=(vmem_spec,) * 4,
        scratch_shapes=[scratch[name] for name in names],
        compiler_params=pltpu.CompilerParams(
            collective_id=0, has_side_effects=True, vmem_limit_bytes=VMEM_LIMIT
        ),
    )(
        *(
            pltpu.with_memory_space_constraint(x, pltpu.HBM)
            for x in (
                grad.reshape((devices, block, LANES)),
                grad.reshape(sizes + (block, LANES)),
                to_rows(master_params),
                to_rows(first_moment),
                to_rows(second_moment),
            )
        )
    )
    results = write_out(new_master, new_first, new_second, weights.reshape(devices * block, LANES))
    return tuple(from_rows(x, layers) for x in results)


def solution(mesh):
    digits = digits_of(mesh.shape["row"], mesh.shape["col"])
    in_specs = (
        P(("row", "col"), None, None),
        P(None, ("row", "col")),
        P(None, ("row", "col")),
        P(None, ("row", "col")),
    )
    out_specs = (P(None, ("row", "col")), P(None, ("row", "col")), P(None, ("row", "col")), P())
    return jax.shard_map(
        functools.partial(shards, digits), mesh=mesh, in_specs=in_specs, out_specs=out_specs, check_vma=False
    )
```
